32 devices in a mesh: gx: 4 (over y, core), gy: 8 (over z, x).
Axes of the slice: x: 2, y: 2, z: 4, core: 2. Of those that a mesh axis runs over, the one named last changes fastest.
Arguments:
- thermal_anomaly: float32 [64, 256, 1024], P(None, 'gx', 'gy'), may hold values from -6 to 6
- eastward_shift_ratio: float32 [64, 256, 1024], P(None, 'gx', 'gy'), may hold values from -0.6 to 0.6
- northward_shift_ratio: float32 [64, 256, 1024], P(None, 'gx', 'gy'), may hold values from -0.6 to 0.6
- upward_shift_ratio: float32 [64, 256, 1024], P(None, 'gx', 'gy'), may hold values from -0.6 to 0.6
- emitted_power: float32 [16, 65536], P(None, ('gx', 'gy')), may hold values from 0.2 to 1
- albedo_values: float32 [16, 65536], P(None, ('gx', 'gy')), may hold values from 0.1 to 0.8
- visibility_matrices: bfloat16 [32, 32, 2, 128, 128], P(('gx', 'gy')), may hold values from 0 to 1
- active_pairing_totals: int32 [32, 32], P(('gx', 'gy')), may hold values from 1 to 2, as said below
- sender_panel_group: int32 [32, 32, 2], P(('gx', 'gy')), may hold values from 0 to 15
- receiver_panel_group: int32 [32, 32, 2], P(None, ('gx', 'gy')), may hold values from 0 to 15
- nearest_ground_index: int32 [65536], P(('gx', 'gy')), may hold values from 0 to 11519
Outputs:
- renewed_thermal_anomaly: float32 [64, 256, 1024], P(None, 'gx', 'gy')
- leaving_power: float32 [16, 65536], P(None, ('gx', 'gy'))
The draws below stay inside these ranges and needn't reach their ends.
Inputs may be any that keep to these rules, and one draw needn't show every extreme that they name: `active_pairing_totals`: in every draw some receiving devices get 2 live slots from every sending device. `sender_panel_group`: A local block index of the sending device. `receiver_panel_group`: A local block index of the receiving device; slots that are not live may hold any index. `nearest_ground_index`: index (x * 144 + y) in the owner's block of cells widened by 8 cells on each side.
All inputs are finite; a program needn't handle non-finite values.
Results may differ from the reference program's by a relative error of at most 0.0003.
Values sent between devices are 32-bit elements; how exact they have to be, the bound alone decides.
No kernel may reach another device: no remote copies, remote signals or barrier semaphores. Data moves between devices by JAX's collectives and lax.ppermute only.
A program may use at most 128 MiB of HBM per device.

```python
import jax
import jax.numpy as jnp
from jax import lax

CX = 64
CY = 128
LEVEL_TOTAL = 64
BANDS = 16
BLK = 128
FB = 16
CAP = 2
MARGIN = 8
NODES = 32
GRID_WIDE_EAST = 256
GRID_WIDE_NORTH = 1024
NFACES = 65536
N_GY = 8


def draw_active_pairing_totals(key, part):
    base_key = jax.random.fold_in(key, 11)
    fewer = jax.random.randint(jax.random.fold_in(base_key, 1), (NODES, NODES), 0, 8) == 0
    drawn = jnp.where(fewer, CAP - 1, CAP)
    popular = jax.random.randint(jax.random.fold_in(base_key, 2), (NODES,), 0, 4) == 0
    chosen = jax.random.randint(jax.random.fold_in(base_key, 3), (), 0, NODES)
    popular = jnp.logical_or(popular, jnp.arange(NODES) == chosen)
    return jnp.where(popular[None, :], CAP, drawn).astype(jnp.int32)


def with_ends(array, key, smallest, top_value):
    place = [jax.random.randint(jax.random.fold_in(key, axis), (), 0, length) for axis, length in enumerate(array.shape)]
    widest = array.shape.index(max(array.shape))
    beside = place[:widest] + [(place[widest] + 1) % array.shape[widest]] + place[widest + 1:]
    return array.at[tuple(place)].set(smallest).at[tuple(beside)].set(top_value)


def shard_levels(key, extent, pieces, smallest, high):
    def one(position, shards_of):
        heights = jax.random.uniform(jax.random.fold_in(jax.random.fold_in(key, 6), position), (shards_of,), jnp.float32, smallest / len(pieces), high / len(pieces))
        return jnp.repeat(jnp.exp(heights), extent[position] // shards_of).reshape((-1,) + (1,) * (len(extent) - position - 1))

    level = one(*pieces[0])
    for cut in pieces[1:]:
        level = level * one(*cut)
    return level


def centred(key, shape, width, reach, shards=(), dtype=jnp.bfloat16):
    entries = jax.random.normal(key, shape, jnp.float32) * width
    if len(shards) > 0:
        entries = shard_levels(key, shape, shards, -0.22, 0.18) * entries
    return jnp.clip(entries, min=-reach, max=reach).astype(dtype)


def setup_inputs(seed: int = 0) -> dict:
    keys = jax.random.split(jax.random.key(seed), 12)
    return {
        "thermal_anomaly": centred(keys[0], (LEVEL_TOTAL, GRID_WIDE_EAST, GRID_WIDE_NORTH), 1.0, 6.0, ((1, 4), (2, 8)), jnp.float32),
        "eastward_shift_ratio": jnp.clip(jax.random.uniform(keys[1], (LEVEL_TOTAL, GRID_WIDE_EAST, GRID_WIDE_NORTH), jnp.float32, -0.6, 0.6) * shard_levels(keys[1], (LEVEL_TOTAL, GRID_WIDE_EAST, GRID_WIDE_NORTH), ((1, 4), (2, 8)), -0.4, 0.0), -0.6, 0.6),
        "northward_shift_ratio": jnp.clip(jax.random.uniform(keys[2], (LEVEL_TOTAL, GRID_WIDE_EAST, GRID_WIDE_NORTH), jnp.float32, -0.6, 0.6) * shard_levels(keys[2], (LEVEL_TOTAL, GRID_WIDE_EAST, GRID_WIDE_NORTH), ((1, 4), (2, 8)), -0.4, 0.0), -0.6, 0.6),
        "upward_shift_ratio": jnp.clip(jax.random.uniform(keys[3], (LEVEL_TOTAL, GRID_WIDE_EAST, GRID_WIDE_NORTH), jnp.float32, -0.6, 0.6) * shard_levels(keys[3], (LEVEL_TOTAL, GRID_WIDE_EAST, GRID_WIDE_NORTH), ((1, 4), (2, 8)), -0.4, 0.0), -0.6, 0.6),
        "emitted_power": jnp.clip(0.2 + 0.8 * jax.random.uniform(keys[4], (BANDS, NFACES), jnp.float32) ** shard_levels(keys[4], (BANDS, NFACES), ((1, 32),), -0.2, 0.2), 0.2, 1.0),
        "albedo_values": jnp.clip(0.1 + 0.7 * jax.random.uniform(keys[5], (BANDS, NFACES), jnp.float32) ** shard_levels(keys[5], (BANDS, NFACES), ((1, 32),), -0.2, 0.2), 0.1, 0.8),
        "visibility_matrices": jnp.clip(1.0 * jax.random.uniform(keys[6], (NODES, NODES, CAP, BLK, BLK), jnp.float32) ** shard_levels(keys[6], (NODES, NODES, CAP, BLK, BLK), ((0, 32),), -0.2, 0.2), 0.0, 1.0).astype(jnp.bfloat16),
        "active_pairing_totals": draw_active_pairing_totals(jax.random.fold_in(keys[11], 71), 0),
        "sender_panel_group": with_ends(jax.random.randint(keys[8], (NODES, NODES, CAP), 0, FB), jax.random.fold_in(keys[8], 1), 0, FB - 1).astype(jnp.int32),
        "receiver_panel_group": with_ends(jax.random.randint(keys[9], (NODES, NODES, CAP), 0, FB), jax.random.fold_in(keys[9], 1), 0, FB - 1).astype(jnp.int32),
        "nearest_ground_index": with_ends(jax.random.randint(keys[10], (NFACES,), 0, (CX + 2 * MARGIN) * (CY + 2 * MARGIN)), jax.random.fold_in(keys[10], 1), 0, ((CX + 2 * MARGIN) * (CY + 2 * MARGIN)) - 1).astype(jnp.int32),
    }


heat_gain = 0.02


def upwind(behind_two, behind_one, center, ahead_one, ahead_two, velocity):
    rising = (behind_two - 6.0 * behind_one + 3.0 * center + 2.0 * ahead_one) / 6.0
    falling = (-2.0 * behind_one - 3.0 * center + 6.0 * ahead_one - ahead_two) / 6.0
    return jnp.where(velocity >= 0.0, rising, falling)


def vertical(transported_quantity, velocity):
    levels = transported_quantity.shape[0]
    padded = jnp.pad(transported_quantity, ((2, 2), (0, 0), (0, 0)), mode="edge")
    return upwind(padded[0:levels], padded[1:levels + 1], padded[2:levels + 2],
                  padded[3:levels + 3], padded[4:levels + 4], velocity)


def carried_change(transported_quantity, eastward_shift_ratio, northward_shift_ratio, upward_shift_ratio):
    along_x = upwind(jnp.roll(transported_quantity, 2, 1), jnp.roll(transported_quantity, 1, 1), transported_quantity,
                     jnp.roll(transported_quantity, -1, 1), jnp.roll(transported_quantity, -2, 1), eastward_shift_ratio)
    along_y = upwind(jnp.roll(transported_quantity, 2, 2), jnp.roll(transported_quantity, 1, 2), transported_quantity,
                     jnp.roll(transported_quantity, -1, 2), jnp.roll(transported_quantity, -2, 2), northward_shift_ratio)
    return -(eastward_shift_ratio * along_x + northward_shift_ratio * along_y + upward_shift_ratio * vertical(transported_quantity, upward_shift_ratio))


def irradiance(light, visibility_matrices, active_pairing_totals, sender_panel_group, receiver_panel_group):
    owned = light.astype(jnp.bfloat16).reshape(BANDS, NODES, FB, BLK)
    slots_live = (jnp.arange(CAP)[None, None, :] < active_pairing_totals[:, :, None]).astype(jnp.float32)

    def sender(total, items):
        local, blocks, source, live, target = items
        chosen = jnp.take(local, source, axis=1).astype(jnp.float32)
        sent = jnp.einsum("krci,rcij->rckj", chosen, blocks.astype(jnp.float32),
                          precision=lax.Precision.HIGHEST)
        sent = sent * (0.5 / BLK) * live[:, :, None, None]
        slots = (target[:, :, None] == jnp.arange(FB)[None, None, :]).astype(jnp.float32)
        total = total + jnp.einsum("rcf,rckj->krfj", slots, sent, precision=lax.Precision.HIGHEST)
        return total, None

    start = jnp.zeros((BANDS, NODES, FB, BLK), jnp.float32)
    total, _ = lax.scan(sender, start, (owned.transpose(1, 0, 2, 3), visibility_matrices, sender_panel_group,
                                        slots_live, receiver_panel_group))
    return total.reshape(BANDS, NODES * FB * BLK)


def reference(thermal_anomaly, eastward_shift_ratio, northward_shift_ratio, upward_shift_ratio, emitted_power, albedo_values, visibility_matrices,
              active_pairing_totals, sender_panel_group, receiver_panel_group, nearest_ground_index):
    first_light = irradiance(emitted_power, visibility_matrices, active_pairing_totals, sender_panel_group, receiver_panel_group)
    bounced = emitted_power + albedo_values * first_light
    second_light = irradiance(bounced, visibility_matrices, active_pairing_totals, sender_panel_group, receiver_panel_group)
    leaving_power = emitted_power + albedo_values * second_light
    absorbed = heat_gain * jnp.sum((1.0 - albedo_values) * second_light, axis=0)
    faces_device = FB * BLK
    face_index = jnp.arange(NODES * faces_device).astype(jnp.int32)
    owners = face_index // faces_device
    span_y = CY + 2 * MARGIN
    cell_x = (owners // N_GY) * CX + nearest_ground_index // span_y - MARGIN
    cell_y = (owners % N_GY) * CY + nearest_ground_index % span_y - MARGIN
    flat_cell = ((cell_x % GRID_WIDE_EAST) * GRID_WIDE_NORTH + cell_y % GRID_WIDE_NORTH).astype(jnp.int32)
    ground_energy_transfer = jax.ops.segment_sum(absorbed, flat_cell, num_segments=GRID_WIDE_EAST * GRID_WIDE_NORTH).reshape(GRID_WIDE_EAST, GRID_WIDE_NORTH)
    initial_reflected_share = thermal_anomaly + carried_change(thermal_anomaly, eastward_shift_ratio, northward_shift_ratio, upward_shift_ratio) / 3.0
    repeated_reflected_share = thermal_anomaly + carried_change(initial_reflected_share, eastward_shift_ratio, northward_shift_ratio, upward_shift_ratio) / 2.0
    advanced_thermal_state = thermal_anomaly + carried_change(repeated_reflected_share, eastward_shift_ratio, northward_shift_ratio, upward_shift_ratio)
    renewed_thermal_anomaly = advanced_thermal_state.at[0].add(ground_energy_transfer)
    return renewed_thermal_anomaly, leaving_power
```

```python
import functools

import jax
import jax.numpy as jnp
from jax import lax
from jax.experimental import pallas as pl
from jax.experimental.pallas import tpu as pltpu
from jax.sharding import PartitionSpec as P


MARGIN = 8
HEAT_GAIN = 0.02
SUB = 8
LANES = 128
EDGE = 4
PIECES = 4

VMEM = pl.BlockSpec(memory_space=pltpu.VMEM)
SMEM = pl.BlockSpec(memory_space=pltpu.SMEM)
HBM = pl.BlockSpec(memory_space=pltpu.HBM)


def swap_low(axis):
    return [(i, i ^ 1) for i in range(lax.axis_size(axis))]


def swap_high(axis):
    count = lax.axis_size(axis)
    return [(i, (i + 1 if i % 2 else i - 1) % count) for i in range(count)]


def is_even(axis):
    return lax.rem(lax.axis_index(axis), 2) == 0


def in_hbm(array):
    return pltpu.with_memory_space_constraint(array, pltpu.HBM)


def grant(mebibytes):
    return pltpu.CompilerParams(vmem_limit_bytes=mebibytes * 1024 * 1024)


def cost(flops, nbytes):
    return pl.CostEstimate(flops=flops, bytes_accessed=nbytes, transcendentals=0)


def lane_group():
    return lax.broadcasted_iota(jnp.int32, (SUB, LANES), 1) // EDGE


def pack_kernel(levels_per, q_hbm, n_hbm, qp_ref, np_ref, edge_a_ref, edge_b_ref, q_ref, n_ref, low_ref, high_ref, sems):
    levels, rows, _ = q_ref.shape
    tiles = rows // SUB
    groups = levels // levels_per
    group_of = lane_group()

    def copies(g):
        at = pl.ds(g * levels_per, levels_per)
        return (
            pltpu.make_async_copy(q_hbm.at[at], q_ref.at[at], sems.at[0, g]),
            pltpu.make_async_copy(n_hbm.at[at], n_ref.at[at], sems.at[1, g]),
        )

    @pl.loop(0, groups)
    def _(g):
        for copy in copies(g):
            copy.start()

    @pl.loop(0, groups)
    def _(g):
        for copy in copies(g):
            copy.wait()
        packed_q = jnp.zeros((SUB, LANES), jnp.float32)
        packed_n = jnp.zeros((SUB, LANES), jnp.float32)
        for t in range(tiles):
            for j in range(levels_per):
                k = t * levels_per + j
                level = g * levels_per + j
                mine = group_of == k
                q = q_ref[level, t * SUB : (t + 1) * SUB, :]
                n = n_ref[level, t * SUB : (t + 1) * SUB, :]
                turn = (EDGE * k + 2) % LANES
                packed_q = jnp.where(mine, pltpu.roll(q, turn, 1), packed_q)
                packed_n = jnp.where(mine, pltpu.roll(n, turn, 1), packed_n)
                at = pl.ds(pl.multiple_of(g * 2 * levels_per, 2 * levels_per) + 2 * j, 2)
                if t == 0:
                    low_ref[at, :] = q[0:2]
                if t == tiles - 1:
                    high_ref[at, :] = q[SUB - 2 : SUB]
        at = pl.ds(pl.multiple_of(g * SUB, SUB), SUB)
        qp_ref[at, :] = packed_q
        np_ref[at, :] = packed_n

    share_edges(edge_a_ref, edge_b_ref, low_ref, high_ref)


def share_edges(edge_a_ref, edge_b_ref, low_ref, high_ref):
    even = is_even("gx")
    edge_a_ref[...] = jnp.where(even, high_ref[...], low_ref[...])
    edge_b_ref[...] = jnp.where(even, low_ref[...], high_ref[...])


def levels_per_group(rows):
    return LANES // EDGE // (rows // SUB)


def pack(q, n):
    levels, rows, columns = q.shape
    per = levels_per_group(rows)
    packed = jax.ShapeDtypeStruct((levels // per * SUB, LANES), jnp.float32)
    edge = jax.ShapeDtypeStruct((levels * 2, columns), jnp.float32)
    return pl.pallas_call(
        functools.partial(pack_kernel, per),
        out_shape=(packed, packed, edge, edge),
        in_specs=[HBM, HBM],
        out_specs=(VMEM, VMEM, VMEM, VMEM),
        scratch_shapes=[
            pltpu.VMEM(q.shape, jnp.float32),
            pltpu.VMEM(q.shape, jnp.float32),
            pltpu.VMEM(edge.shape, jnp.float32),
            pltpu.VMEM(edge.shape, jnp.float32),
            pltpu.SemaphoreType.DMA((2, levels // per)),
        ],
        name="pack",
        compiler_params=grant(6),
        cost_estimate=cost(4_000_000, q.size * 8),
    )(in_hbm(q), in_hbm(n))


def stage_kernel(
    levels_per, coefficient, first_stage, last, base_hbm, q_hbm, e_hbm, n_hbm, u_hbm,
    edge_a_in, edge_b_in, own_ref, side_a_ref, side_b_ref, np_ref, out_hbm, *rest,
):
    if last:
        ground_ref, padded, base_ref, e_ref, n_ref, u_ref, out_ref, sems, done = rest
    else:
        packed_ref, edge_a_ref, edge_b_ref, padded, base_ref, e_ref, n_ref, u_ref, out_ref, low_ref, high_ref, sems, done = rest
    levels, rows, _ = out_ref.shape
    tiles = rows // SUB
    groups = levels // levels_per
    lane = lax.broadcasted_iota(jnp.int32, (SUB, LANES), 1)
    group_of = lane // EDGE
    member = lane % EDGE
    touched = jnp.logical_or(lane < 2, lane >= LANES - 2)
    even_x, even_y = is_even("gx"), is_even("gy")

    def field(g):
        at = pl.ds(g * levels_per, levels_per)
        return pltpu.make_async_copy(q_hbm.at[at], padded.at[at, pl.ds(SUB, rows)], sems.at[0, g])

    def others(g):
        at = pl.ds(g * levels_per, levels_per)
        found = [
            pltpu.make_async_copy(e_hbm.at[at], e_ref.at[at], sems.at[1, g]),
            pltpu.make_async_copy(n_hbm.at[at], n_ref.at[at], sems.at[2, g]),
            pltpu.make_async_copy(u_hbm.at[at], u_ref.at[at], sems.at[3, g]),
        ]
        if not first_stage:
            found.append(pltpu.make_async_copy(base_hbm.at[at], base_ref.at[at], sems.at[4, g]))
        return found

    def outgoing(g):
        at = pl.ds(g * levels_per, levels_per)
        return pltpu.make_async_copy(out_ref.at[at], out_hbm.at[at], done.at[g])

    @pl.loop(0, groups)
    def _(g):
        field(g).start()
        for copy in others(g):
            copy.start()

    field(0).wait()

    @pl.loop(0, groups)
    def _(g):
        @pl.when(g + 1 < groups)
        def _():
            field(g + 1).wait()

        for copy in others(g):
            copy.wait()
        for j in range(levels_per):
            level = g * levels_per + j
            rows_at = pl.ds(pl.multiple_of(g * 2 * levels_per, 2 * levels_per) + 2 * j, 2)
            got_a, got_b = edge_a_in[rows_at, :], edge_b_in[rows_at, :]
            padded[level, SUB - 2 : SUB, :] = jnp.where(even_x, got_b, got_a)
            padded[level, SUB + rows : SUB + rows + 2, :] = jnp.where(even_x, got_a, got_b)
        at = pl.ds(pl.multiple_of(g * SUB, SUB), SUB)
        side_a, side_b = side_a_ref[at, :], side_b_ref[at, :]
        right = jnp.where(even_y, side_a, side_b)
        left = jnp.where(even_y, side_b, side_a)
        own = own_ref[at, :]
        speed = np_ref[at, :]
        gap = jnp.where(
            member < 2,
            pltpu.roll(right - own, LANES - 2, 1),
            pltpu.roll(left - own, 2, 1),
        )
        before = pltpu.roll(gap, 1, 1)
        after = pltpu.roll(gap, LANES - 1, 1)
        rising = jnp.where(
            member == 0, 0.0, jnp.where(member == 1, 2.0 * before, jnp.where(member == 2, gap - 6.0 * after, gap))
        )
        falling = jnp.where(
            member == 0, gap, jnp.where(member == 1, gap - 6.0 * before, jnp.where(member == 2, 2.0 * after, 0.0))
        )
        mend = jnp.abs(speed) * jnp.where(speed >= 0.0, rising, falling)
        packed = jnp.zeros((SUB, LANES), jnp.float32)
        first = g * levels_per
        for t in range(tiles):
            here = slice(SUB + t * SUB, SUB + (t + 1) * SUB)
            tile = slice(t * SUB, (t + 1) * SUB)
            column = []
            for d in range(-2, levels_per + 2):
                level = first + d
                if d < 0:
                    level = jnp.maximum(level, 0)
                elif d >= levels_per:
                    level = jnp.minimum(level, levels - 1)
                column.append(padded[level, here, :])
            for j in range(levels_per):
                k = t * levels_per + j
                level = first + j
                q = column[j + 2]
                triple = 3.0 * q

                def moved(back_two, back, ahead, ahead_two, velocity):
                    positive = velocity >= 0.0
                    near = jnp.where(positive, back, ahead)
                    far = jnp.where(positive, back_two, ahead_two)
                    return jnp.abs(velocity) * (
                        (far - 8.0 * near) + (2.0 * (back + ahead) + triple)
                    )

                def row(offset):
                    return padded[level, SUB + t * SUB + offset : SUB + (t + 1) * SUB + offset, :]

                total = moved(row(-2), row(-1), row(1), row(2), e_ref[level, tile, :])
                total += moved(column[j], column[j + 1], column[j + 3], column[j + 4], u_ref[level, tile, :])
                total += moved(
                    pltpu.roll(q, 2, 1),
                    pltpu.roll(q, 1, 1),
                    pltpu.roll(q, LANES - 1, 1),
                    pltpu.roll(q, LANES - 2, 1),
                    n_ref[level, tile, :],
                )
                total += jnp.where(touched, pltpu.roll(mend, (2 * LANES - 2 - EDGE * k) % LANES, 1), 0.0)
                base = q if first_stage else base_ref[level, tile, :]
                result = base - (coefficient / 6.0) * total
                out_ref[level, tile, :] = result
                if last:
                    continue
                packed = jnp.where(group_of == k, pltpu.roll(result, (EDGE * k + 2) % LANES, 1), packed)
                edge_at = pl.ds(pl.multiple_of(g * 2 * levels_per, 2 * levels_per) + 2 * j, 2)
                if t == 0:
                    low_ref[edge_at, :] = result[0:2]
                if t == tiles - 1:
                    high_ref[edge_at, :] = result[SUB - 2 : SUB]
        if not last:
            packed_ref[at, :] = packed
        outgoing(g).start()

    if last:
        ground_ref[...] = out_ref[0]
    else:
        share_edges(edge_a_ref, edge_b_ref, low_ref, high_ref)

    @pl.loop(0, groups)
    def _(g):
        outgoing(g).wait()


def stage(base, q, winds, edges, packed_winds, coefficient, first_stage=False, last=False):
    levels, rows, columns = q.shape
    per = levels_per_group(rows)
    whole = pltpu.HBM(q.shape, jnp.float32)
    packed = jax.ShapeDtypeStruct((levels // per * SUB, LANES), jnp.float32)
    edge = jax.ShapeDtypeStruct((levels * 2, columns), jnp.float32)
    ground = jax.ShapeDtypeStruct((rows, columns), jnp.float32)
    outs = (whole, ground) if last else (whole, packed, edge, edge)
    return pl.pallas_call(
        functools.partial(stage_kernel, per, coefficient, first_stage, last),
        out_shape=outs,
        in_specs=[HBM] * 5 + [VMEM] * 6,
        out_specs=(HBM,) + (VMEM,) * (len(outs) - 1),
        scratch_shapes=[
            pltpu.VMEM((levels, rows + 2 * SUB, columns), jnp.float32),
            pltpu.VMEM((SUB, LANES) if first_stage else q.shape, jnp.float32),
            *(pltpu.VMEM(q.shape, jnp.float32) for _ in range(4)),
            *(pltpu.VMEM(edge.shape, jnp.float32) for _ in range(0 if last else 2)),
            pltpu.SemaphoreType.DMA((5, levels // per)),
            pltpu.SemaphoreType.DMA((levels // per,)),
        ],
        name="stage",
        compiler_params=grant(16),
        cost_estimate=cost(24_000_000, q.size * 24),
    )(*map(in_hbm, (base, q, *winds)), *edges, packed_winds)


def swap(array, axis):
    a = lax.ppermute(array[0], axis, swap_low(axis))
    b = lax.ppermute(array[1], axis, swap_high(axis))
    return a, b


def neighbours(packed, edge_a, edge_b):
    sides = swap((packed, packed), "gy")
    edges = swap((edge_a, edge_b), "gx")
    return *edges, packed, *sides


def exchange(sent):
    return lax.all_to_all(sent, ("gx", "gy"), split_axis=0, concat_axis=0, tiled=True)


def project(light, blocks_ref, source_ref, live_ref, sent_hbm, sent_ref, done, ready=None):
    peers, slots, width, _ = blocks_ref.shape
    bands = light.shape[1]
    nothing = jnp.zeros((bands, width), jnp.bfloat16)
    pieces = done.shape[0]
    share = peers // pieces

    def outgoing(p):
        at = pl.ds(p * share, share)
        return pltpu.make_async_copy(sent_ref.at[at], sent_hbm.at[at], done.at[p])

    for p in range(pieces):
        if ready is not None:
            ready(p)

        @pl.loop(p * share, (p + 1) * share, unroll=4)
        def _(r):
            for c in range(0, slots, 2):
                one = light[source_ref[c, r]]
                two = light[source_ref[c + 1, r]]
                left = jnp.concatenate(
                    [jnp.concatenate([one, nothing], axis=1), jnp.concatenate([nothing, two], axis=1)], axis=0
                )
                right = blocks_ref[r, c : c + 2].reshape(2 * width, width)
                got = jnp.dot(left, right, preferred_element_type=jnp.float32)
                for d in range(2):
                    scale = jnp.where(c + d < live_ref[0, r], 0.5 / width, 0.0)
                    sent_ref[r, c + d] = got[d * bands : (d + 1) * bands] * scale

        outgoing(p).start()
    for p in range(pieces):
        outgoing(p).wait()


def first_kernel(emitted_ref, blocks_ref, source_ref, live_ref, sent_hbm, light, sent_ref, done):
    blocks, _, width = light.shape
    for f in range(blocks):
        light[f] = emitted_ref[:, f * width : (f + 1) * width].astype(jnp.bfloat16)
    project(light, blocks_ref, source_ref, live_ref, sent_hbm, sent_ref, done)


def gather_light(arrived_ref, target_ref, total):
    peers, slots = arrived_ref.shape[:2]
    total[...] = jnp.zeros_like(total)

    @pl.loop(0, peers, unroll=4)
    def _(s):
        for c in range(slots):
            g = target_ref[c, s]
            total[g] = total[g] + arrived_ref[s, c]


def second_kernel(
    arrived_ref, target_ref, emitted_ref, albedo_ref, blocks_hbm, source_ref, live_ref, sent_hbm,
    light, total, blocks_ref, sent_ref, done, loaded,
):
    pieces = loaded.shape[0]
    share = blocks_ref.shape[0] // pieces

    def incoming(p):
        at = pl.ds(p * share, share)
        return pltpu.make_async_copy(blocks_hbm.at[at], blocks_ref.at[at], loaded.at[p])

    for p in range(pieces):
        incoming(p).start()
    gather_light(arrived_ref, target_ref, total)
    blocks, _, width = light.shape
    for f in range(blocks):
        at = slice(f * width, (f + 1) * width)
        light[f] = (emitted_ref[:, at] + albedo_ref[:, at] * total[f]).astype(jnp.bfloat16)
    project(light, blocks_ref, source_ref, live_ref, sent_hbm, sent_ref, done, lambda p: incoming(p).wait())


def last_kernel(
    rows, columns, arrived_ref, target_ref, emitted_ref, albedo_ref, ground_ref,
    leaving_ref, inner_ref, rim_a_ref, rim_b_ref, total, heat, cells,
):
    gather_light(arrived_ref, target_ref, total)
    blocks, _, width = total.shape
    span_x, span_y = rows + 2 * MARGIN, columns + 2 * MARGIN
    x_index = lax.broadcasted_iota(jnp.int32, (span_x, width), 0).astype(jnp.float32)
    y_index = lax.broadcasted_iota(jnp.int32, (2 * columns, width), 0).astype(jnp.float32)
    for f in range(blocks):
        at = slice(f * width, (f + 1) * width)
        light = total[f]
        albedo = albedo_ref[:, at]
        leaving_ref[:, at] = emitted_ref[:, at] + albedo * light
        absorbed = HEAT_GAIN * jnp.sum((1.0 - albedo) * light, axis=0, keepdims=True)
        place = ground_ref[f : f + 1, :].astype(jnp.float32)
        x = jnp.floor((place + 0.5) * (1.0 / span_y))
        y = place - span_y * x
        x = jnp.where(x < MARGIN, x + (span_x - MARGIN), x - MARGIN)
        y = jnp.where(y < MARGIN, y + (2 * columns - MARGIN), y - MARGIN)
        coarse = absorbed.astype(jnp.bfloat16).astype(jnp.float32)
        fine = absorbed - coarse
        hit = x_index == x
        heat[0:span_x, at] = jnp.where(hit, coarse, 0.0).astype(jnp.bfloat16)
        heat[span_x : 2 * span_x, at] = jnp.where(hit, fine, 0.0).astype(jnp.bfloat16)
        cells[:, at] = jnp.where(y_index == y, 1.0, 0.0).astype(jnp.bfloat16)
    both = lax.dot_general(
        heat[...], cells[...], (((1,), (1,)), ((), ())), preferred_element_type=jnp.float32
    )
    field = both[0:span_x] + both[span_x : 2 * span_x]
    inner_ref[...] = field[0:rows]
    upper = field[rows : rows + MARGIN]
    lower = field[rows + MARGIN : rows + 2 * MARGIN]
    even = is_even("gx")
    rim_a_ref[...] = jnp.where(even, upper, lower)
    rim_b_ref[...] = jnp.where(even, lower, upper)


def fold_kernel(inner_ref, rim_a_ref, rim_b_ref, middle_ref, side_ref):
    rows, columns = middle_ref.shape
    even = is_even("gx")
    for half, ref in ((0, middle_ref), (1, side_ref)):
        at = slice(half * columns, (half + 1) * columns)
        rim_a, rim_b = rim_a_ref[:, at], rim_b_ref[:, at]
        ref[...] = inner_ref[:, at]
        ref[0:MARGIN, :] = ref[0:MARGIN, :] + jnp.where(even, rim_b, rim_a)
        ref[rows - MARGIN : rows, :] = ref[rows - MARGIN : rows, :] + jnp.where(even, rim_a, rim_b)


def finish_kernel(field_ref, ground_ref, middle_ref, side_a_ref, side_b_ref, out_ref, level, sem):
    lane = lax.broadcasted_iota(jnp.int32, level.shape, 1)
    columns = level.shape[1]
    even = is_even("gy")
    left = jnp.where(even, side_b_ref[...], side_a_ref[...])
    right = jnp.where(even, side_a_ref[...], side_b_ref[...])
    level[...] = (
        ground_ref[...]
        + middle_ref[...]
        + jnp.where(lane < MARGIN, left, 0.0)
        + jnp.where(lane >= columns - MARGIN, right, 0.0)
    )
    copy = pltpu.make_async_copy(level, out_ref.at[0], sem)
    copy.start()
    copy.wait()


def step(
    thermal_anomaly,
    eastward_shift_ratio,
    northward_shift_ratio,
    upward_shift_ratio,
    emitted_power,
    albedo_values,
    visibility_matrices,
    active_pairing_totals,
    sender_panel_group,
    receiver_panel_group,
    nearest_ground_index,
):
    _, rows, columns = thermal_anomaly.shape
    bands, faces = emitted_power.shape
    blocks = visibility_matrices[0]
    peers, slots, width, _ = blocks.shape
    owned = faces // width
    source = jnp.transpose(sender_panel_group[0])
    target = jnp.transpose(receiver_panel_group[:, 0, :])
    message = pltpu.HBM((peers, slots, bands, width), jnp.float32)
    light = pltpu.VMEM((owned, bands, width), jnp.bfloat16)
    total = pltpu.VMEM((owned, bands, width), jnp.float32)
    winds = (eastward_shift_ratio, northward_shift_ratio, upward_shift_ratio)

    sent = pl.pallas_call(
        first_kernel,
        out_shape=message,
        in_specs=[VMEM, VMEM, SMEM, SMEM],
        out_specs=HBM,
        scratch_shapes=[light, pltpu.VMEM(message.shape, jnp.float32), pltpu.SemaphoreType.DMA((PIECES,))],
        name="first",
        compiler_params=grant(4),
        cost_estimate=cost(10_000_000, blocks.size * 2),
    )(emitted_power, blocks, source, active_pairing_totals)
    packed, packed_winds, *rows_sent = pack(thermal_anomaly, northward_shift_ratio)
    edges = neighbours(packed, *rows_sent)
    arrived = exchange(sent)

    one, *sides = stage(thermal_anomaly, thermal_anomaly, winds, edges, packed_winds, 1.0 / 3.0, first_stage=True)
    edges = neighbours(*sides)

    sent = pl.pallas_call(
        second_kernel,
        out_shape=message,
        in_specs=[VMEM, SMEM, VMEM, VMEM, HBM, SMEM, SMEM],
        out_specs=HBM,
        scratch_shapes=[
            light,
            total,
            pltpu.VMEM(blocks.shape, jnp.bfloat16),
            pltpu.VMEM(message.shape, jnp.float32),
            pltpu.SemaphoreType.DMA((PIECES,)),
            pltpu.SemaphoreType.DMA((PIECES,)),
        ],
        name="second",
        compiler_params=grant(6 + 6 * peers // 32),
        cost_estimate=cost(12_000_000, blocks.size * 2),
    )(arrived, target, emitted_power, albedo_values, in_hbm(blocks), source, active_pairing_totals)
    arrived = exchange(sent)

    two, *sides = stage(thermal_anomaly, one, winds, edges, packed_winds, 1.0 / 2.0)
    edges = neighbours(*sides)

    span_x = rows + 2 * MARGIN
    rim = jax.ShapeDtypeStruct((MARGIN, 2 * columns), jnp.float32)
    leaving, inner, *rims = pl.pallas_call(
        functools.partial(last_kernel, rows, columns),
        out_shape=(
            jax.ShapeDtypeStruct((bands, faces), jnp.float32),
            jax.ShapeDtypeStruct((rows, 2 * columns), jnp.float32),
            rim,
            rim,
        ),
        in_specs=[VMEM, SMEM, VMEM, VMEM, VMEM],
        out_specs=(VMEM,) * 4,
        scratch_shapes=[
            total,
            pltpu.VMEM((2 * span_x, faces), jnp.bfloat16),
            pltpu.VMEM((2 * columns, faces), jnp.bfloat16),
        ],
        name="last",
        compiler_params=grant(8),
        cost_estimate=cost(16_000_000, arrived.size * 4),
    )(arrived, target, emitted_power, albedo_values, nearest_ground_index.reshape(owned, width))
    rims = swap(rims, "gx")

    three, ground = stage(thermal_anomaly, two, winds, edges, packed_winds, 1.0, last=True)

    flat = jax.ShapeDtypeStruct((rows, columns), jnp.float32)
    middle, side = pl.pallas_call(
        fold_kernel,
        out_shape=(flat, flat),
        in_specs=[VMEM] * 3,
        out_specs=(VMEM, VMEM),
        name="fold",
        compiler_params=grant(2),
        cost_estimate=cost(500_000, flat.size * 8),
    )(inner, *rims)
    sides = swap((side, side), "gy")

    renewed = pl.pallas_call(
        finish_kernel,
        out_shape=jax.ShapeDtypeStruct(thermal_anomaly.shape, jnp.float32),
        in_specs=[HBM, VMEM, VMEM, VMEM, VMEM],
        out_specs=HBM,
        scratch_shapes=[pltpu.VMEM((rows, columns), jnp.float32), pltpu.SemaphoreType.DMA],
        input_output_aliases={0: 0},
        name="finish",
        compiler_params=grant(2),
        cost_estimate=cost(500_000, flat.size * 8),
    )(three, ground, middle, *sides)
    return renewed, leaving


def solution(mesh):
    in_specs = (
        P(None, "gx", "gy"),
        P(None, "gx", "gy"),
        P(None, "gx", "gy"),
        P(None, "gx", "gy"),
        P(None, ("gx", "gy")),
        P(None, ("gx", "gy")),
        P(("gx", "gy"), None, None, None, None),
        P(("gx", "gy"), None),
        P(("gx", "gy"), None, None),
        P(None, ("gx", "gy"), None),
        P(("gx", "gy")),
    )
    out_specs = (P(None, "gx", "gy"), P(None, ("gx", "gy")))
    return jax.shard_map(step, mesh=mesh, in_specs=in_specs, out_specs=out_specs, check_vma=False)
```

```python
import functools

import jax
import jax.numpy as jnp
from jax import lax
from jax.experimental import pallas as pl
from jax.experimental.pallas import tpu as pltpu
from jax.sharding import PartitionSpec as P


MARGIN = 8
HEAT_GAIN = 0.02
SUB = 8
LANES = 128
PIECES = 4
BULKS = 8

VMEM = pl.BlockSpec(memory_space=pltpu.VMEM)
SMEM = pl.BlockSpec(memory_space=pltpu.SMEM)
HBM = pl.BlockSpec(memory_space=pltpu.HBM)


def swap_low(axis):
    return [(i, i ^ 1) for i in range(lax.axis_size(axis))]


def swap_high(axis):
    count = lax.axis_size(axis)
    return [(i, (i + 1 if i % 2 else i - 1) % count) for i in range(count)]


def is_even(axis):
    return lax.rem(lax.axis_index(axis), 2) == 0


def in_hbm(array):
    return pltpu.with_memory_space_constraint(array, pltpu.HBM)


def grant(mebibytes):
    return pltpu.CompilerParams(vmem_limit_bytes=mebibytes * 1024 * 1024)


def cost(flops, nbytes):
    return pl.CostEstimate(flops=flops, bytes_accessed=nbytes, transcendentals=0)


def bulk_copies(pairs, sems, b):
    found = []
    for i, (source, target) in enumerate(pairs):
        deep = source.shape[0] // sems.shape[1]
        at = pl.ds(b * deep, deep)
        target = target.at[at]
        if target.shape != source.at[at].shape:
            target = target.at[:, pl.ds(SUB, source.shape[1])]
        found.append(pltpu.make_async_copy(source.at[at], target, sems.at[i, b]))
    return found


def edge_rows(b, count, i):
    return pl.ds(pl.multiple_of(b * 2 * count, 2 * count) + 2 * i, 2)


def share_edges(axis, edge_a_ref, edge_b_ref, low_ref, high_ref):
    even = is_even(axis)
    edge_a_ref[...] = jnp.where(even, high_ref[...], low_ref[...])
    edge_b_ref[...] = jnp.where(even, low_ref[...], high_ref[...])


def edge_shapes(shape):
    levels, rows, columns = shape
    x = jax.ShapeDtypeStruct((levels * 2, columns), jnp.float32)
    y = jax.ShapeDtypeStruct((levels * rows // LANES * 2, LANES), jnp.float32)
    return x, x, y, y


def edge_scratch(shape):
    return [pltpu.VMEM(edge.shape, edge.dtype) for edge in edge_shapes(shape)]


def keep_edges(b, i, count, fold, rows_of, turned, x_low, x_high, y_low, y_high):
    columns = turned.shape[0]
    for j, rows in enumerate(rows_of):
        x_low[edge_rows(b, count * fold, i * fold + j), :] = rows[0:2]
        x_high[edge_rows(b, count * fold, i * fold + j), :] = rows[-2:]
    y_low[edge_rows(b, count, i), :] = turned[0:2]
    y_high[edge_rows(b, count, i), :] = turned[columns - 2 : columns]


def opening_kernel(
    q_hbm, emitted_hbm, blocks_hbm, source_hbm, live_hbm, xa_ref, xb_ref, ya_ref, yb_ref, sent_hbm,
    x_low, x_high, y_low, y_high, q_ref, emitted_ref, blocks_ref, source_ref, live_ref, light, sent_ref, sems, loaded, done, lit,
):
    levels, rows, columns = q_ref.shape
    bulks = sems.shape[1]
    fold = LANES // rows
    count = levels // bulks // fold

    def copies(b):
        return bulk_copies([(q_hbm, q_ref)], sems, b)

    small = [
        pltpu.make_async_copy(source, target, lit.at[i])
        for i, (source, target) in enumerate(
            ((emitted_hbm, emitted_ref), (source_hbm, source_ref), (live_hbm, live_ref))
        )
    ]
    for copy in small:
        copy.start()
    for b in range(bulks):
        copies(b)[0].start()
    for b in range(loaded.shape[1]):
        bulk_copies([(blocks_hbm, blocks_ref)], loaded, b)[0].start()

    @pl.loop(0, bulks)
    def _(b):
        copies(b)[0].wait()
        for i in range(count):
            q = q_ref[pl.ds((b * count + i) * fold, fold)]
            turned = q.reshape(fold * rows, columns).T
            keep_edges(b, i, count, fold, [q[j] for j in range(fold)], turned, x_low, x_high, y_low, y_high)

    share_edges("gx", xa_ref, xb_ref, x_low, x_high)
    share_edges("gy", ya_ref, yb_ref, y_low, y_high)
    for copy in small:
        copy.wait()
    owned, _, width = light.shape
    for f in range(owned):
        light[f] = emitted_ref[:, f * width : (f + 1) * width].astype(jnp.bfloat16)
    project(
        light, blocks_ref, source_ref, live_ref, sent_hbm, sent_ref, done,
        lambda b: bulk_copies([(blocks_hbm, blocks_ref)], loaded, b)[0].wait(),
    )


def opening(q, emitted, blocks, source, live, message, light):
    return pl.pallas_call(
        opening_kernel,
        out_shape=(*edge_shapes(q.shape), message),
        in_specs=[HBM] * 5,
        out_specs=(*(VMEM,) * 4, HBM),
        scratch_shapes=[
            *edge_scratch(q.shape),
            pltpu.VMEM(q.shape, jnp.float32),
            pltpu.VMEM(emitted.shape, jnp.float32),
            pltpu.VMEM(blocks.shape, jnp.bfloat16),
            pltpu.SMEM(source.shape, jnp.int32),
            pltpu.SMEM(live.shape, jnp.int32),
            light,
            pltpu.VMEM(message.shape, jnp.float32),
            pltpu.SemaphoreType.DMA((1, BULKS)),
            pltpu.SemaphoreType.DMA((1, PIECES)),
            pltpu.SemaphoreType.DMA((PIECES,)),
            pltpu.SemaphoreType.DMA((3,)),
        ],
        name="opening",
        compiler_params=grant(8 + 5 * blocks.shape[0] // 32),
        cost_estimate=cost(12_000_000, q.size * 4 + blocks.size * 2),
    )(*map(in_hbm, (q, emitted, blocks, source, live)))


def moved(back_two, back, center, ahead, ahead_two, velocity):
    positive = velocity >= 0.0
    near = jnp.where(positive, back, ahead)
    far = jnp.where(positive, back_two, ahead_two)
    return jnp.abs(velocity) * ((far - 8.0 * near) + (2.0 * (back + ahead) + 3.0 * center))


def stage_kernel(
    coefficient, first_stage, last, begin, end, base_hbm, q_hbm, e_hbm, n_hbm, u_hbm,
    xa_in, xb_in, ya_in, yb_in, *rest,
):
    if begin > 0:
        _, *rest = rest
    out_hbm, *rest = rest
    if last:
        if begin == 0:
            ground_ref, *rest = rest
    else:
        xa_ref, xb_ref, ya_ref, yb_ref, *rest = rest
    if first_stage:
        speed_hbm, *rest = rest
    x_low, x_high, y_low, y_high, padded, turned, base_ref, e_ref, n_ref, u_ref, out_ref, *rest = rest
    speed_ref = n_ref
    if first_stage:
        speed_ref, *rest = rest
    sems, done = rest
    levels, rows, columns = out_ref.shape
    tiles = rows // SUB
    bulks = sems.shape[1]
    fold = LANES // rows
    count = levels // bulks // fold

    def field(b):
        return bulk_copies([(q_hbm, padded)], sems, b)

    def others(b):
        found = [(e_hbm, e_ref), (n_hbm, n_ref), (u_hbm, u_ref)]
        if not first_stage:
            found.append((base_hbm, base_ref))
        return bulk_copies([(q_hbm, padded)] + found, sems, b)[1:]

    def outgoing(b):
        found = [(out_ref, out_hbm)]
        if first_stage:
            found.append((speed_ref, speed_hbm))
        return bulk_copies(found, done, b)

    below, above = max(begin - 1, 0), min(end + 1, bulks)
    for b in range(below, above):
        for copy in field(b):
            copy.start()
    for b in range(begin, end):
        for copy in others(b):
            copy.start()
    even_x, even_y = is_even("gx"), is_even("gy")

    @pl.loop(begin, end)
    def _(b):
        for copy in field(b):
            copy.wait()
        for i in range(count):
            p = b * count + i
            for j in range(fold):
                level = p * fold + j
                at = edge_rows(b, count * fold, i * fold + j)
                got_a, got_b = xa_in[at, :], xb_in[at, :]
                padded[level, SUB - 2 : SUB, :] = jnp.where(even_x, got_b, got_a)
                padded[level, SUB + rows : SUB + rows + 2, :] = jnp.where(even_x, got_a, got_b)
            at = edge_rows(b, count, i)
            got_a, got_b = ya_in[at, :], yb_in[at, :]
            turned[p, SUB - 2 : SUB, :] = jnp.where(even_y, got_b, got_a)
            turned[p, SUB + columns : SUB + columns + 2, :] = jnp.where(even_y, got_a, got_b)
            q = padded[pl.ds(p * fold, fold), SUB : SUB + rows, :]
            turned[p, SUB : SUB + columns, :] = q.reshape(fold * rows, columns).T

    for b in [*range(below, begin), *range(end, above)]:
        for copy in field(b):
            copy.wait()

    @pl.loop(begin, end)
    def _(b):
        for copy in others(b):
            copy.wait()
        for i in range(count):
            p = b * count + i
            if first_stage:
                speed_ref[p] = n_ref[pl.ds(p * fold, fold)].reshape(fold * rows, columns).T
            terms = []
            for t in range(columns // SUB):

                def line(offset):
                    return turned[p, SUB + t * SUB + offset : 2 * SUB + t * SUB + offset, :]

                terms.append(
                    moved(line(-2), line(-1), line(0), line(1), line(2), speed_ref[p, t * SUB : (t + 1) * SUB, :])
                )
            along_y = jnp.concatenate(terms, axis=0).T
            results = [[] for _ in range(fold)]
            for t in range(tiles):
                tile = slice(t * SUB, (t + 1) * SUB)
                column = []
                for d in range(-2, fold + 2):
                    level = p * fold + d
                    if i * fold + d < 0:
                        level = jnp.maximum(level, 0)
                    elif i * fold + d >= count * fold:
                        level = jnp.minimum(level, levels - 1)
                    column.append(padded[level, SUB + t * SUB : 2 * SUB + t * SUB, :])
                for j in range(fold):
                    level = p * fold + j

                    def row(offset):
                        return padded[level, SUB + t * SUB + offset : 2 * SUB + t * SUB + offset, :]

                    q = column[j + 2]
                    total = moved(row(-2), row(-1), q, row(1), row(2), e_ref[level, tile, :])
                    total += moved(*column[j : j + 5], u_ref[level, tile, :])
                    total += along_y[j * rows + t * SUB : j * rows + (t + 1) * SUB]
                    base = q if first_stage else base_ref[level, tile, :]
                    result = base - (coefficient / 6.0) * total
                    out_ref[level, tile, :] = result
                    results[j].append(result)
            if not last:
                found = [jnp.concatenate(part, axis=0) for part in results]
                keep_edges(
                    b, i, count, fold, found, jnp.concatenate(found, axis=0).T, x_low, x_high, y_low, y_high
                )
        for copy in outgoing(b):
            copy.start()

    if last:
        if begin == 0:
            ground_ref[...] = out_ref[0]
    else:
        share_edges("gx", xa_ref, xb_ref, x_low, x_high)
        share_edges("gy", ya_ref, yb_ref, y_low, y_high)
    for b in range(begin, end):
        for copy in outgoing(b):
            copy.wait()


def stage(base, q, winds, edges, coefficient, first_stage=False, last=False, begin=0, end=BULKS, started=None):
    levels, rows, columns = q.shape
    blocks = levels * rows // LANES
    whole = pltpu.HBM(q.shape, jnp.float32)
    ground = jax.ShapeDtypeStruct((rows, columns), jnp.float32)
    outs = (whole, *(() if last else edge_shapes(q.shape)))
    outs += (ground,) if last and begin == 0 else ()
    outs += (pltpu.HBM((blocks, columns, LANES), jnp.float32),) if first_stage else ()
    field = pltpu.VMEM(q.shape, jnp.float32)
    turned = pltpu.VMEM((blocks, columns, LANES), jnp.float32)
    return pl.pallas_call(
        functools.partial(stage_kernel, coefficient, first_stage, last, begin, end),
        out_shape=outs,
        in_specs=[HBM] * 5 + [VMEM] * 4 + [HBM] * (begin > 0),
        input_output_aliases={9: 0} if begin > 0 else {},
        out_specs=tuple(HBM if isinstance(out, type(whole)) else VMEM for out in outs),
        scratch_shapes=[
            *edge_scratch(q.shape),
            pltpu.VMEM((levels, rows + 2 * SUB, columns), jnp.float32),
            pltpu.VMEM((blocks, columns + 2 * SUB, LANES), jnp.float32),
            pltpu.VMEM((SUB, LANES), jnp.float32) if first_stage else field,
            field,
            field if first_stage else turned,
            field,
            field,
            *([turned] if first_stage else []),
            pltpu.SemaphoreType.DMA((5, BULKS)),
            pltpu.SemaphoreType.DMA((2, BULKS)),
        ],
        name="stage",
        compiler_params=grant(20),
        cost_estimate=cost(24_000_000 * (end - begin) // BULKS, q.size * 24 * (end - begin) // BULKS),
    )(*map(in_hbm, (base, q, *winds)), *edges, *([started] if begin > 0 else []))


def swap(array, axis):
    a = lax.ppermute(array[0], axis, swap_low(axis))
    b = lax.ppermute(array[1], axis, swap_high(axis))
    return a, b


def neighbours(x_low, x_high, y_low, y_high):
    y_edges = swap((y_low, y_high), "gy")
    x_edges = swap((x_low, x_high), "gx")
    return *x_edges, *y_edges


def exchange(sent):
    return lax.all_to_all(sent, ("gx", "gy"), split_axis=0, concat_axis=0, tiled=True)


def project(light, blocks_ref, source_ref, live_ref, sent_hbm, sent_ref, done, ready=None):
    peers, slots, width, _ = blocks_ref.shape
    bands = light.shape[1]
    nothing = jnp.zeros((bands, width), jnp.bfloat16)
    pieces = done.shape[0]
    share = peers // pieces

    def outgoing(p):
        at = pl.ds(p * share, share)
        return pltpu.make_async_copy(sent_ref.at[at], sent_hbm.at[at], done.at[p])

    for p in range(pieces):
        if ready is not None:
            ready(p)

        @pl.loop(p * share, (p + 1) * share, unroll=4)
        def _(r):
            for c in range(0, slots, 2):
                one = light[source_ref[c, r]]
                two = light[source_ref[c + 1, r]]
                left = jnp.concatenate(
                    [jnp.concatenate([one, nothing], axis=1), jnp.concatenate([nothing, two], axis=1)], axis=0
                )
                right = blocks_ref[r, c : c + 2].reshape(2 * width, width)
                got = jnp.dot(left, right, preferred_element_type=jnp.float32)
                for d in range(2):
                    scale = jnp.where(c + d < live_ref[0, r], 0.5 / width, 0.0)
                    sent_ref[r, c + d] = got[d * bands : (d + 1) * bands] * scale

        outgoing(p).start()
    for p in range(pieces):
        outgoing(p).wait()


def gather_light(arrived_ref, target_ref, total):
    peers, slots = arrived_ref.shape[:2]
    total[...] = jnp.zeros_like(total)

    @pl.loop(0, peers, unroll=4)
    def _(s):
        for c in range(slots):
            g = target_ref[c, s]
            total[g] = total[g] + arrived_ref[s, c]


def second_kernel(
    arrived_ref, target_ref, emitted_ref, albedo_ref, blocks_hbm, source_ref, live_ref, sent_hbm,
    light, total, blocks_ref, sent_ref, done, loaded,
):
    pieces = loaded.shape[0]
    share = blocks_ref.shape[0] // pieces

    def incoming(p):
        at = pl.ds(p * share, share)
        return pltpu.make_async_copy(blocks_hbm.at[at], blocks_ref.at[at], loaded.at[p])

    for p in range(pieces):
        incoming(p).start()
    gather_light(arrived_ref, target_ref, total)
    blocks, _, width = light.shape
    for f in range(blocks):
        at = slice(f * width, (f + 1) * width)
        light[f] = (emitted_ref[:, at] + albedo_ref[:, at] * total[f]).astype(jnp.bfloat16)
    project(light, blocks_ref, source_ref, live_ref, sent_hbm, sent_ref, done, lambda p: incoming(p).wait())


def last_kernel(
    rows, columns, arrived_ref, target_ref, emitted_ref, albedo_ref, ground_ref,
    leaving_ref, inner_ref, rim_a_ref, rim_b_ref, total, heat, cells,
):
    gather_light(arrived_ref, target_ref, total)
    blocks, _, width = total.shape
    span_x, span_y = rows + 2 * MARGIN, columns + 2 * MARGIN
    x_index = lax.broadcasted_iota(jnp.int32, (span_x, width), 0).astype(jnp.float32)
    y_index = lax.broadcasted_iota(jnp.int32, (2 * columns, width), 0).astype(jnp.float32)
    for f in range(blocks):
        at = slice(f * width, (f + 1) * width)
        light = total[f]
        albedo = albedo_ref[:, at]
        leaving_ref[:, at] = emitted_ref[:, at] + albedo * light
        absorbed = HEAT_GAIN * jnp.sum((1.0 - albedo) * light, axis=0, keepdims=True)
        place = ground_ref[f : f + 1, :].astype(jnp.float32)
        x = jnp.floor((place + 0.5) * (1.0 / span_y))
        y = place - span_y * x
        x = jnp.where(x < MARGIN, x + (span_x - MARGIN), x - MARGIN)
        y = jnp.where(y < MARGIN, y + (2 * columns - MARGIN), y - MARGIN)
        coarse = absorbed.astype(jnp.bfloat16).astype(jnp.float32)
        fine = absorbed - coarse
        hit = x_index == x
        heat[0:span_x, at] = jnp.where(hit, coarse, 0.0).astype(jnp.bfloat16)
        heat[span_x : 2 * span_x, at] = jnp.where(hit, fine, 0.0).astype(jnp.bfloat16)
        cells[:, at] = jnp.where(y_index == y, 1.0, 0.0).astype(jnp.bfloat16)
    both = lax.dot_general(
        heat[...], cells[...], (((1,), (1,)), ((), ())), preferred_element_type=jnp.float32
    )
    field = both[0:span_x] + both[span_x : 2 * span_x]
    inner_ref[...] = field[0:rows]
    upper = field[rows : rows + MARGIN]
    lower = field[rows + MARGIN : rows + 2 * MARGIN]
    even = is_even("gx")
    rim_a_ref[...] = jnp.where(even, upper, lower)
    rim_b_ref[...] = jnp.where(even, lower, upper)


def fold_kernel(inner_ref, rim_a_ref, rim_b_ref, middle_ref, side_ref):
    rows, columns = middle_ref.shape
    even = is_even("gx")
    for half, ref in ((0, middle_ref), (1, side_ref)):
        at = slice(half * columns, (half + 1) * columns)
        rim_a, rim_b = rim_a_ref[:, at], rim_b_ref[:, at]
        ref[...] = inner_ref[:, at]
        ref[0:MARGIN, :] = ref[0:MARGIN, :] + jnp.where(even, rim_b, rim_a)
        ref[rows - MARGIN : rows, :] = ref[rows - MARGIN : rows, :] + jnp.where(even, rim_a, rim_b)


def finish_kernel(field_ref, ground_ref, middle_ref, side_a_ref, side_b_ref, out_ref, level, sem):
    lane = lax.broadcasted_iota(jnp.int32, level.shape, 1)
    columns = level.shape[1]
    even = is_even("gy")
    left = jnp.where(even, side_b_ref[...], side_a_ref[...])
    right = jnp.where(even, side_a_ref[...], side_b_ref[...])
    level[...] = (
        ground_ref[...]
        + middle_ref[...]
        + jnp.where(lane < MARGIN, left, 0.0)
        + jnp.where(lane >= columns - MARGIN, right, 0.0)
    )
    copy = pltpu.make_async_copy(level, out_ref.at[0], sem)
    copy.start()
    copy.wait()


def step(
    thermal_anomaly,
    eastward_shift_ratio,
    northward_shift_ratio,
    upward_shift_ratio,
    emitted_power,
    albedo_values,
    visibility_matrices,
    active_pairing_totals,
    sender_panel_group,
    receiver_panel_group,
    nearest_ground_index,
):
    _, rows, columns = thermal_anomaly.shape
    bands, faces = emitted_power.shape
    blocks = visibility_matrices[0]
    peers, slots, width, _ = blocks.shape
    owned = faces // width
    source = jnp.transpose(sender_panel_group[0])
    target = jnp.transpose(receiver_panel_group[:, 0, :])
    message = pltpu.HBM((peers, slots, bands, width), jnp.float32)
    light = pltpu.VMEM((owned, bands, width), jnp.bfloat16)
    total = pltpu.VMEM((owned, bands, width), jnp.float32)
    winds = (eastward_shift_ratio, northward_shift_ratio, upward_shift_ratio)

    *edges, sent = opening(
        thermal_anomaly, emitted_power, blocks, source, active_pairing_totals, message, light
    )
    edges = neighbours(*edges)
    arrived = exchange(sent)

    one, *sides, speed = stage(thermal_anomaly, thermal_anomaly, winds, edges, 1.0 / 3.0, first_stage=True)
    winds = (eastward_shift_ratio, speed, upward_shift_ratio)
    edges = neighbours(*sides)

    sent = pl.pallas_call(
        second_kernel,
        out_shape=message,
        in_specs=[VMEM, SMEM, VMEM, VMEM, HBM, SMEM, SMEM],
        out_specs=HBM,
        scratch_shapes=[
            light,
            total,
            pltpu.VMEM(blocks.shape, jnp.bfloat16),
            pltpu.VMEM(message.shape, jnp.float32),
            pltpu.SemaphoreType.DMA((PIECES,)),
            pltpu.SemaphoreType.DMA((PIECES,)),
        ],
        name="second",
        compiler_params=grant(6 + 6 * peers // 32),
        cost_estimate=cost(12_000_000, blocks.size * 2),
    )(arrived, target, emitted_power, albedo_values, in_hbm(blocks), source, active_pairing_totals)
    arrived = exchange(sent)

    two, *sides = stage(thermal_anomaly, one, winds, edges, 1.0 / 2.0)
    edges = neighbours(*sides)

    span_x = rows + 2 * MARGIN
    rim = jax.ShapeDtypeStruct((MARGIN, 2 * columns), jnp.float32)
    leaving, inner, *rims = pl.pallas_call(
        functools.partial(last_kernel, rows, columns),
        out_shape=(
            jax.ShapeDtypeStruct((bands, faces), jnp.float32),
            jax.ShapeDtypeStruct((rows, 2 * columns), jnp.float32),
            rim,
            rim,
        ),
        in_specs=[VMEM, SMEM, VMEM, VMEM, VMEM],
        out_specs=(VMEM,) * 4,
        scratch_shapes=[
            total,
            pltpu.VMEM((2 * span_x, faces), jnp.bfloat16),
            pltpu.VMEM((2 * columns, faces), jnp.bfloat16),
        ],
        name="last",
        compiler_params=grant(8),
        cost_estimate=cost(16_000_000, arrived.size * 4),
    )(arrived, target, emitted_power, albedo_values, nearest_ground_index.reshape(owned, width))
    rims = swap(rims, "gx")

    three, ground = stage(thermal_anomaly, two, winds, edges, 1.0, last=True)

    flat = jax.ShapeDtypeStruct((rows, columns), jnp.float32)
    middle, side = pl.pallas_call(
        fold_kernel,
        out_shape=(flat, flat),
        in_specs=[VMEM] * 3,
        out_specs=(VMEM, VMEM),
        name="fold",
        compiler_params=grant(2),
        cost_estimate=cost(500_000, flat.size * 8),
    )(inner, *rims)
    sides = swap((side, side), "gy")

    renewed = pl.pallas_call(
        finish_kernel,
        out_shape=jax.ShapeDtypeStruct(thermal_anomaly.shape, jnp.float32),
        in_specs=[HBM, VMEM, VMEM, VMEM, VMEM],
        out_specs=HBM,
        scratch_shapes=[pltpu.VMEM((rows, columns), jnp.float32), pltpu.SemaphoreType.DMA],
        input_output_aliases={0: 0},
        name="finish",
        compiler_params=grant(2),
        cost_estimate=cost(500_000, flat.size * 8),
    )(three, ground, middle, *sides)
    return renewed, leaving


def solution(mesh):
    in_specs = (
        P(None, "gx", "gy"),
        P(None, "gx", "gy"),
        P(None, "gx", "gy"),
        P(None, "gx", "gy"),
        P(None, ("gx", "gy")),
        P(None, ("gx", "gy")),
        P(("gx", "gy"), None, None, None, None),
        P(("gx", "gy"), None),
        P(("gx", "gy"), None, None),
        P(None, ("gx", "gy"), None),
        P(("gx", "gy")),
    )
    out_specs = (P(None, "gx", "gy"), P(None, ("gx", "gy")))
    return jax.shard_map(step, mesh=mesh, in_specs=in_specs, out_specs=out_specs, check_vma=False)
```

```python
import functools
from typing import NamedTuple

import jax
import jax.numpy as jnp
from jax import lax
from jax.experimental import pallas as pl
from jax.experimental.pallas import tpu as pltpu
from jax.sharding import PartitionSpec as P


MARGIN = 8
HEAT_GAIN = 0.02
SUB = 8
LANES = 128
PIECES = 4
BULKS = 4
FIRST_BULKS = 2

VMEM = pl.BlockSpec(memory_space=pltpu.VMEM)
SMEM = pl.BlockSpec(memory_space=pltpu.SMEM)
HBM = pl.BlockSpec(memory_space=pltpu.HBM)


def swap_low(axis):
    return [(i, i ^ 1) for i in range(lax.axis_size(axis))]


def swap_high(axis):
    count = lax.axis_size(axis)
    return [(i, (i + 1 if i % 2 else i - 1) % count) for i in range(count)]


def is_even(axis):
    return lax.rem(lax.axis_index(axis), 2) == 0


def in_hbm(array):
    return pltpu.with_memory_space_constraint(array, pltpu.HBM)


def grant(mebibytes):
    return pltpu.CompilerParams(vmem_limit_bytes=mebibytes * 1024 * 1024)


def cost(flops, nbytes):
    return pl.CostEstimate(flops=flops, bytes_accessed=nbytes, transcendentals=0)


def bulk_copies(pairs, sems, b):
    found = []
    for i, (source, target) in enumerate(pairs):
        deep = source.shape[0] // sems.shape[1]
        at = pl.ds(b * deep, deep)
        target = target.at[at]
        if target.shape != source.at[at].shape:
            target = target.at[:, pl.ds(SUB, source.shape[1])]
        found.append(pltpu.make_async_copy(source.at[at], target, sems.at[i, b]))
    return found


def edge_rows(b, count, i):
    return pl.ds(pl.multiple_of(b * 2 * count, 2 * count) + 2 * i, 2)


def share_edges(axis, edge_a_ref, edge_b_ref, low_ref, high_ref):
    even = is_even(axis)
    edge_a_ref[...] = jnp.where(even, high_ref[...], low_ref[...])
    edge_b_ref[...] = jnp.where(even, low_ref[...], high_ref[...])


def edge_shapes(shape):
    levels, rows, columns = shape
    x = jax.ShapeDtypeStruct((levels * 2, columns), jnp.float32)
    y = jax.ShapeDtypeStruct((levels * rows // LANES * 2, LANES), jnp.float32)
    return x, x, y, y


def edge_scratch(shape):
    return [pltpu.VMEM(edge.shape, edge.dtype) for edge in edge_shapes(shape)]


def keep_edges(b, i, count, fold, rows_of, turned, x_low, x_high, y_low, y_high):
    columns = turned.shape[0]
    for j, rows in enumerate(rows_of):
        x_low[edge_rows(b, count * fold, i * fold + j), :] = rows[0:2]
        x_high[edge_rows(b, count * fold, i * fold + j), :] = rows[-2:]
    y_low[edge_rows(b, count, i), :] = turned[0:2]
    y_high[edge_rows(b, count, i), :] = turned[columns - 2 : columns]


def opening_kernel(
    q_hbm, emitted_hbm, blocks_hbm, source_hbm, live_hbm, xa_ref, xb_ref, ya_ref, yb_ref, sent_hbm,
    x_low, x_high, y_low, y_high, q_ref, emitted_ref, blocks_ref, source_ref, live_ref, light, sent_ref, sems, loaded, done, lit,
):
    levels, rows, columns = q_ref.shape
    bulks = sems.shape[1]
    fold = LANES // rows
    count = levels // bulks // fold

    def copies(b):
        return bulk_copies([(q_hbm, q_ref)], sems, b)

    small = [
        pltpu.make_async_copy(source, target, lit.at[i])
        for i, (source, target) in enumerate(
            ((emitted_hbm, emitted_ref), (source_hbm, source_ref), (live_hbm, live_ref))
        )
    ]
    for copy in small:
        copy.start()
    for b in range(loaded.shape[1]):
        bulk_copies([(blocks_hbm, blocks_ref)], loaded, b)[0].start()
    for b in range(bulks):
        copies(b)[0].start()
    for copy in small:
        copy.wait()
    owned, _, width = light.shape
    for f in range(owned):
        light[f] = emitted_ref[:, f * width : (f + 1) * width].astype(jnp.bfloat16)
    finish = project(
        light, blocks_ref, source_ref, live_ref, sent_hbm, sent_ref, done,
        lambda b: bulk_copies([(blocks_hbm, blocks_ref)], loaded, b)[0].wait(),
    )

    @pl.loop(0, bulks)
    def _(b):
        copies(b)[0].wait()
        for i in range(count):
            q = q_ref[pl.ds((b * count + i) * fold, fold)]
            turned = q.reshape(fold * rows, columns).T
            keep_edges(b, i, count, fold, [q[j] for j in range(fold)], turned, x_low, x_high, y_low, y_high)

    share_edges("gx", xa_ref, xb_ref, x_low, x_high)
    share_edges("gy", ya_ref, yb_ref, y_low, y_high)
    finish()


def opening(q, emitted, blocks, source, live, message, light):
    return pl.pallas_call(
        opening_kernel,
        out_shape=(*edge_shapes(q.shape), message),
        in_specs=[HBM] * 5,
        out_specs=(*(VMEM,) * 4, HBM),
        scratch_shapes=[
            *edge_scratch(q.shape),
            pltpu.VMEM(q.shape, jnp.float32),
            pltpu.VMEM(emitted.shape, jnp.float32),
            pltpu.VMEM(blocks.shape, jnp.bfloat16),
            pltpu.SMEM(source.shape, jnp.int32),
            pltpu.SMEM(live.shape, jnp.int32),
            light,
            pltpu.VMEM(message.shape, jnp.float32),
            pltpu.SemaphoreType.DMA((1, FIRST_BULKS)),
            pltpu.SemaphoreType.DMA((1, PIECES)),
            pltpu.SemaphoreType.DMA((PIECES,)),
            pltpu.SemaphoreType.DMA((3,)),
        ],
        name="opening",
        compiler_params=grant(8 + 5 * blocks.shape[0] // 32),
        cost_estimate=cost(12_000_000, q.size * 4 + blocks.size * 2),
    )(*map(in_hbm, (q, emitted, blocks, source, live)))


def moved(back_two, back, center, ahead, ahead_two, velocity):
    positive = velocity >= 0.0
    near = jnp.where(positive, back, ahead)
    far = jnp.where(positive, back_two, ahead_two)
    return jnp.abs(velocity) * ((far - 8.0 * near) + (2.0 * (back + ahead) + 3.0 * center))


def stage_kernel(coefficient, plan, *refs):
    refs = list(refs)

    def take(count, wanted=True):
        return [refs.pop(0) for _ in range(count)] if wanted else [None] * count

    (q_hbm,) = take(1)
    (base_hbm,) = take(1, plan.own_base)
    e_hbm, u_hbm = take(2, plan.xz)
    (n_hbm,) = take(1, plan.y)
    xa_in, xb_in = take(2, plan.xz)
    ya_in, yb_in = take(2, plan.y)
    (out_hbm,) = take(1)
    xa_ref, xb_ref, ya_ref, yb_ref = take(4, plan.shares)
    (speed_hbm,) = take(1, plan.turns)
    (ground_ref,) = take(1, plan.ground)
    padded, out_ref, sems, done = take(4)
    x_low, x_high, y_low, y_high = take(4, plan.shares)
    (base_ref,) = take(1, plan.own_base)
    e_ref, u_ref = take(2, plan.xz)
    turned, speed_ref = take(2, plan.y)
    (n_ref,) = take(1, plan.turns)

    levels, rows, columns = out_ref.shape
    tiles = rows // SUB
    bulks = sems.shape[1]
    fold = LANES // rows
    count = levels // bulks // fold

    def field(b):
        return bulk_copies([(q_hbm, padded)], sems, b)

    def others(b):
        found = []
        if plan.xz:
            found += [(e_hbm, e_ref), (u_hbm, u_ref)]
        if plan.y:
            found.append((n_hbm, n_ref if plan.turns else speed_ref))
        if plan.own_base:
            found.append((base_hbm, base_ref))
        return [
            pltpu.make_async_copy(
                source.at[pl.ds(b * (source.shape[0] // bulks), source.shape[0] // bulks)],
                target.at[pl.ds(b * (source.shape[0] // bulks), source.shape[0] // bulks)],
                sems.at[i + 1, b],
            )
            for i, (source, target) in enumerate(found)
        ]

    def outgoing(b):
        found = [(out_ref, out_hbm)]
        if plan.turns:
            found.append((speed_ref, speed_hbm))
        return bulk_copies(found, done, b)

    for b in range(bulks):
        for copy in field(b):
            copy.start()
    for b in range(bulks):
        for copy in others(b):
            copy.start()
    even_x, even_y = is_even("gx"), is_even("gy")

    @pl.loop(0, bulks)
    def _(b):
        for copy in field(b):
            copy.wait()
        for i in range(count):
            p = b * count + i
            for j in range(fold if plan.xz else 0):
                level = p * fold + j
                at = edge_rows(b, count * fold, i * fold + j)
                got_a, got_b = xa_in[at, :], xb_in[at, :]
                padded[level, SUB - 2 : SUB, :] = jnp.where(even_x, got_b, got_a)
                padded[level, SUB + rows : SUB + rows + 2, :] = jnp.where(even_x, got_a, got_b)
            if plan.y:
                at = edge_rows(b, count, i)
                got_a, got_b = ya_in[at, :], yb_in[at, :]
                turned[p, SUB - 2 : SUB, :] = jnp.where(even_y, got_b, got_a)
                turned[p, SUB + columns : SUB + columns + 2, :] = jnp.where(even_y, got_a, got_b)
                q = padded[pl.ds(p * fold, fold), SUB : SUB + rows, :]
                turned[p, SUB : SUB + columns, :] = q.reshape(fold * rows, columns).T

    @pl.loop(0, bulks)
    def _(b):
        for copy in others(b):
            copy.wait()
        for i in range(count):
            p = b * count + i
            if plan.turns:
                speed_ref[p] = n_ref[pl.ds(p * fold, fold)].reshape(fold * rows, columns).T
            if plan.y:
                terms = []
                for t in range(columns // SUB):

                    def line(offset):
                        return turned[p, SUB + t * SUB + offset : 2 * SUB + t * SUB + offset, :]

                    terms.append(
                        moved(line(-2), line(-1), line(0), line(1), line(2), speed_ref[p, t * SUB : (t + 1) * SUB, :])
                    )
                along_y = jnp.concatenate(terms, axis=0).T
            results = [[] for _ in range(fold)]
            for t in range(tiles):
                tile = slice(t * SUB, (t + 1) * SUB)
                column = []
                for d in range(-2, fold + 2) if plan.xz else ():
                    level = p * fold + d
                    if i * fold + d < 0:
                        level = jnp.maximum(level, 0)
                    elif i * fold + d >= count * fold:
                        level = jnp.minimum(level, levels - 1)
                    column.append(padded[level, SUB + t * SUB : 2 * SUB + t * SUB, :])
                for j in range(fold):
                    level = p * fold + j
                    total = 0.0
                    if plan.xz:

                        def row(offset):
                            return padded[level, SUB + t * SUB + offset : 2 * SUB + t * SUB + offset, :]

                        q = column[j + 2]
                        total = moved(row(-2), row(-1), q, row(1), row(2), e_ref[level, tile, :])
                        total += moved(*column[j : j + 5], u_ref[level, tile, :])
                    if plan.y:
                        total += along_y[j * rows + t * SUB : j * rows + (t + 1) * SUB]
                    base = base_ref[level, tile, :] if plan.own_base else q
                    result = base - (coefficient / 6.0) * total
                    out_ref[level, tile, :] = result
                    results[j].append(result)
            if plan.shares:
                found = [jnp.concatenate(part, axis=0) for part in results]
                keep_edges(
                    b, i, count, fold, found, jnp.concatenate(found, axis=0).T, x_low, x_high, y_low, y_high
                )
        for copy in outgoing(b):
            copy.start()

    if plan.ground:
        ground_ref[...] = out_ref[0]
    if plan.shares:
        share_edges("gx", xa_ref, xb_ref, x_low, x_high)
        share_edges("gy", ya_ref, yb_ref, y_low, y_high)
    for b in range(bulks):
        for copy in outgoing(b):
            copy.wait()


class Plan(NamedTuple):
    xz: bool = True
    y: bool = True
    own_base: bool = True
    shares: bool = True
    turns: bool = False
    ground: bool = False


def stage(plan, coefficient, q, base, winds_xz, wind_y, x_edges, y_edges):
    levels, rows, columns = q.shape
    blocks = levels * rows // LANES
    field = pltpu.VMEM(q.shape, jnp.float32)
    turned = pltpu.VMEM((blocks, columns, LANES), jnp.float32)
    large, small = [q], []
    outs = [pltpu.HBM(q.shape, jnp.float32)]
    scratch = [
        pltpu.VMEM((levels, rows + 2 * SUB, columns), jnp.float32),
        field,
        pltpu.SemaphoreType.DMA((5, BULKS)),
        pltpu.SemaphoreType.DMA((2, BULKS)),
    ]
    if plan.shares:
        outs += edge_shapes(q.shape)
        scratch += edge_scratch(q.shape)
    if plan.own_base:
        large.append(base)
        scratch.append(field)
    if plan.xz:
        large += winds_xz
        small += x_edges
        scratch += [field, field]
    if plan.y:
        large.append(wind_y)
        small += y_edges
        scratch += [pltpu.VMEM((blocks, columns + 2 * SUB, LANES), jnp.float32), turned]
    if plan.turns:
        outs.append(pltpu.HBM((blocks, columns, LANES), jnp.float32))
        scratch.append(field)
    if plan.ground:
        outs.append(jax.ShapeDtypeStruct((rows, columns), jnp.float32))
    return pl.pallas_call(
        functools.partial(stage_kernel, coefficient, plan),
        out_shape=outs,
        in_specs=[HBM] * len(large) + [VMEM] * len(small),
        out_specs=[HBM if isinstance(out, type(outs[0])) else VMEM for out in outs],
        scratch_shapes=scratch,
        name="stage",
        compiler_params=grant(20),
        cost_estimate=cost(24_000_000, q.size * 24),
    )(*map(in_hbm, large), *small)


def swap(array, axis):
    a = lax.ppermute(array[0], axis, swap_low(axis))
    b = lax.ppermute(array[1], axis, swap_high(axis))
    return a, b


def neighbours(x_low, x_high, y_low, y_high):
    y_edges = swap((y_low, y_high), "gy")
    x_edges = swap((x_low, x_high), "gx")
    return x_edges, y_edges


def exchange(sent):
    return lax.all_to_all(sent, ("gx", "gy"), split_axis=0, concat_axis=0, tiled=True)


def project(light, blocks_ref, source_ref, live_ref, sent_hbm, sent_ref, done, ready=None):
    peers, slots, width, _ = blocks_ref.shape
    bands = light.shape[1]
    nothing = jnp.zeros((bands, width), jnp.bfloat16)
    pieces = done.shape[0]
    share = peers // pieces

    def outgoing(p):
        at = pl.ds(p * share, share)
        return pltpu.make_async_copy(sent_ref.at[at], sent_hbm.at[at], done.at[p])

    for p in range(pieces):
        if ready is not None:
            ready(p)

        @pl.loop(p * share, (p + 1) * share, unroll=4)
        def _(r):
            for c in range(0, slots, 2):
                one = light[source_ref[c, r]]
                two = light[source_ref[c + 1, r]]
                left = jnp.concatenate(
                    [jnp.concatenate([one, nothing], axis=1), jnp.concatenate([nothing, two], axis=1)], axis=0
                )
                right = blocks_ref[r, c : c + 2].reshape(2 * width, width)
                got = jnp.dot(left, right, preferred_element_type=jnp.float32)
                for d in range(2):
                    scale = jnp.where(c + d < live_ref[0, r], 0.5 / width, 0.0)
                    sent_ref[r, c + d] = got[d * bands : (d + 1) * bands] * scale

        outgoing(p).start()

    def finish():
        for p in range(pieces):
            outgoing(p).wait()

    return finish


def gather_light(arrived_ref, target_ref, total):
    peers, slots = arrived_ref.shape[:2]
    total[...] = jnp.zeros_like(total)

    @pl.loop(0, peers, unroll=4)
    def _(s):
        for c in range(slots):
            g = target_ref[c, s]
            total[g] = total[g] + arrived_ref[s, c]


def second_kernel(
    arrived_ref, target_ref, emitted_ref, albedo_ref, blocks_hbm, source_ref, live_ref, sent_hbm,
    light, total, blocks_ref, sent_ref, done, loaded,
):
    pieces = loaded.shape[0]
    share = blocks_ref.shape[0] // pieces

    def incoming(p):
        at = pl.ds(p * share, share)
        return pltpu.make_async_copy(blocks_hbm.at[at], blocks_ref.at[at], loaded.at[p])

    for p in range(pieces):
        incoming(p).start()
    gather_light(arrived_ref, target_ref, total)
    blocks, _, width = light.shape
    for f in range(blocks):
        at = slice(f * width, (f + 1) * width)
        light[f] = (emitted_ref[:, at] + albedo_ref[:, at] * total[f]).astype(jnp.bfloat16)
    project(light, blocks_ref, source_ref, live_ref, sent_hbm, sent_ref, done, lambda p: incoming(p).wait())()


def last_kernel(
    rows, columns, arrived_ref, target_ref, emitted_ref, albedo_ref, ground_ref,
    leaving_ref, inner_ref, rim_a_ref, rim_b_ref, total, heat, cells,
):
    gather_light(arrived_ref, target_ref, total)
    blocks, _, width = total.shape
    span_x, span_y = rows + 2 * MARGIN, columns + 2 * MARGIN
    x_index = lax.broadcasted_iota(jnp.int32, (span_x, width), 0).astype(jnp.float32)
    y_index = lax.broadcasted_iota(jnp.int32, (2 * columns, width), 0).astype(jnp.float32)
    for f in range(blocks):
        at = slice(f * width, (f + 1) * width)
        light = total[f]
        albedo = albedo_ref[:, at]
        leaving_ref[:, at] = emitted_ref[:, at] + albedo * light
        absorbed = HEAT_GAIN * jnp.sum((1.0 - albedo) * light, axis=0, keepdims=True)
        place = ground_ref[f : f + 1, :].astype(jnp.float32)
        x = jnp.floor((place + 0.5) * (1.0 / span_y))
        y = place - span_y * x
        x = jnp.where(x < MARGIN, x + (span_x - MARGIN), x - MARGIN)
        y = jnp.where(y < MARGIN, y + (2 * columns - MARGIN), y - MARGIN)
        coarse = absorbed.astype(jnp.bfloat16).astype(jnp.float32)
        fine = absorbed - coarse
        hit = x_index == x
        heat[0:span_x, at] = jnp.where(hit, coarse, 0.0).astype(jnp.bfloat16)
        heat[span_x : 2 * span_x, at] = jnp.where(hit, fine, 0.0).astype(jnp.bfloat16)
        cells[:, at] = jnp.where(y_index == y, 1.0, 0.0).astype(jnp.bfloat16)
    both = lax.dot_general(
        heat[...], cells[...], (((1,), (1,)), ((), ())), preferred_element_type=jnp.float32
    )
    field = both[0:span_x] + both[span_x : 2 * span_x]
    inner_ref[...] = field[0:rows]
    upper = field[rows : rows + MARGIN]
    lower = field[rows + MARGIN : rows + 2 * MARGIN]
    even = is_even("gx")
    rim_a_ref[...] = jnp.where(even, upper, lower)
    rim_b_ref[...] = jnp.where(even, lower, upper)


def fold_kernel(inner_ref, rim_a_ref, rim_b_ref, middle_ref, side_ref):
    rows, columns = middle_ref.shape
    even = is_even("gx")
    for half, ref in ((0, middle_ref), (1, side_ref)):
        at = slice(half * columns, (half + 1) * columns)
        rim_a, rim_b = rim_a_ref[:, at], rim_b_ref[:, at]
        ref[...] = inner_ref[:, at]
        ref[0:MARGIN, :] = ref[0:MARGIN, :] + jnp.where(even, rim_b, rim_a)
        ref[rows - MARGIN : rows, :] = ref[rows - MARGIN : rows, :] + jnp.where(even, rim_a, rim_b)


def finish_kernel(field_ref, ground_ref, middle_ref, side_a_ref, side_b_ref, out_ref, level, sem):
    lane = lax.broadcasted_iota(jnp.int32, level.shape, 1)
    columns = level.shape[1]
    even = is_even("gy")
    left = jnp.where(even, side_b_ref[...], side_a_ref[...])
    right = jnp.where(even, side_a_ref[...], side_b_ref[...])
    level[...] = (
        ground_ref[...]
        + middle_ref[...]
        + jnp.where(lane < MARGIN, left, 0.0)
        + jnp.where(lane >= columns - MARGIN, right, 0.0)
    )
    copy = pltpu.make_async_copy(level, out_ref.at[0], sem)
    copy.start()
    copy.wait()


def step(
    thermal_anomaly,
    eastward_shift_ratio,
    northward_shift_ratio,
    upward_shift_ratio,
    emitted_power,
    albedo_values,
    visibility_matrices,
    active_pairing_totals,
    sender_panel_group,
    receiver_panel_group,
    nearest_ground_index,
):
    _, rows, columns = thermal_anomaly.shape
    bands, faces = emitted_power.shape
    blocks = visibility_matrices[0]
    peers, slots, width, _ = blocks.shape
    owned = faces // width
    source = jnp.transpose(sender_panel_group[0])
    target = jnp.transpose(receiver_panel_group[:, 0, :])
    message = pltpu.HBM((peers, slots, bands, width), jnp.float32)
    light = pltpu.VMEM((owned, bands, width), jnp.bfloat16)
    total = pltpu.VMEM((owned, bands, width), jnp.float32)

    *edges, sent = opening(
        thermal_anomaly, emitted_power, blocks, source, active_pairing_totals, message, light
    )
    edges = neighbours(*edges)
    arrived = exchange(sent)

    winds = (eastward_shift_ratio, upward_shift_ratio)
    one, *sides, speed = stage(
        Plan(own_base=False, turns=True), 1.0 / 3.0, thermal_anomaly, None, winds, northward_shift_ratio, *edges
    )
    edges = neighbours(*sides)

    sent = pl.pallas_call(
        second_kernel,
        out_shape=message,
        in_specs=[VMEM, SMEM, VMEM, VMEM, HBM, SMEM, SMEM],
        out_specs=HBM,
        scratch_shapes=[
            light,
            total,
            pltpu.VMEM(blocks.shape, jnp.bfloat16),
            pltpu.VMEM(message.shape, jnp.float32),
            pltpu.SemaphoreType.DMA((PIECES,)),
            pltpu.SemaphoreType.DMA((PIECES,)),
        ],
        name="second",
        compiler_params=grant(6 + 6 * peers // 32),
        cost_estimate=cost(12_000_000, blocks.size * 2),
    )(arrived, target, emitted_power, albedo_values, in_hbm(blocks), source, active_pairing_totals)
    arrived = exchange(sent)

    two, *sides = stage(Plan(), 1.0 / 2.0, one, thermal_anomaly, winds, speed, *edges)
    edges = neighbours(*sides)
    (part,) = stage(Plan(y=False, shares=False), 1.0, two, thermal_anomaly, winds, None, *edges)

    span_x = rows + 2 * MARGIN
    rim = jax.ShapeDtypeStruct((MARGIN, 2 * columns), jnp.float32)
    leaving, inner, *rims = pl.pallas_call(
        functools.partial(last_kernel, rows, columns),
        out_shape=(
            jax.ShapeDtypeStruct((bands, faces), jnp.float32),
            jax.ShapeDtypeStruct((rows, 2 * columns), jnp.float32),
            rim,
            rim,
        ),
        in_specs=[VMEM, SMEM, VMEM, VMEM, VMEM],
        out_specs=(VMEM,) * 4,
        scratch_shapes=[
            total,
            pltpu.VMEM((2 * span_x, faces), jnp.bfloat16),
            pltpu.VMEM((2 * columns, faces), jnp.bfloat16),
        ],
        name="last",
        compiler_params=grant(8),
        cost_estimate=cost(16_000_000, arrived.size * 4),
    )(arrived, target, emitted_power, albedo_values, nearest_ground_index.reshape(owned, width))
    rims = swap(rims, "gx")

    three, ground = stage(
        Plan(xz=False, shares=False, ground=True), 1.0, two, part, None, speed, *edges
    )

    flat = jax.ShapeDtypeStruct((rows, columns), jnp.float32)
    middle, side = pl.pallas_call(
        fold_kernel,
        out_shape=(flat, flat),
        in_specs=[VMEM] * 3,
        out_specs=(VMEM, VMEM),
        name="fold",
        compiler_params=grant(2),
        cost_estimate=cost(500_000, flat.size * 8),
    )(inner, *rims)
    sides = swap((side, side), "gy")

    renewed = pl.pallas_call(
        finish_kernel,
        out_shape=jax.ShapeDtypeStruct(thermal_anomaly.shape, jnp.float32),
        in_specs=[HBM, VMEM, VMEM, VMEM, VMEM],
        out_specs=HBM,
        scratch_shapes=[pltpu.VMEM((rows, columns), jnp.float32), pltpu.SemaphoreType.DMA],
        input_output_aliases={0: 0},
        name="finish",
        compiler_params=grant(2),
        cost_estimate=cost(500_000, flat.size * 8),
    )(three, ground, middle, *sides)
    return renewed, leaving


def solution(mesh):
    in_specs = (
        P(None, "gx", "gy"),
        P(None, "gx", "gy"),
        P(None, "gx", "gy"),
        P(None, "gx", "gy"),
        P(None, ("gx", "gy")),
        P(None, ("gx", "gy")),
        P(("gx", "gy"), None, None, None, None),
        P(("gx", "gy"), None),
        P(("gx", "gy"), None, None),
        P(None, ("gx", "gy"), None),
        P(("gx", "gy")),
    )
    out_specs = (P(None, "gx", "gy"), P(None, ("gx", "gy")))
    return jax.shard_map(step, mesh=mesh, in_specs=in_specs, out_specs=out_specs, check_vma=False)
```
